32 devices in a mesh: seq: 16 (over z, x, core), tp: 2 (over y).
Axes of the slice: x: 2, y: 2, z: 4, core: 2. Of those that a mesh axis runs over, the one named last changes fastest.
Arguments:
- tokens: bfloat16 [4096, 4096], P('seq', 'tp'), may hold values from -6 to 6
- decay_rate: float32 [4096, 16], P('tp'), as said below
- angle: float32 [4096, 16], P('tp'), may hold values from -3.140625 to 3.140625
- in_coef: float32 [4096, 16], P('tp'), may hold values from -4 to 4
- out_coef: float32 [2, 4096, 16], P(None, 'tp'), may hold values from -1.5 to 1.5
- skip_coef: float32 [4096], P('tp'), may hold values from 0.3 to 1.5
- gate_weight: bfloat16 [4096, 4096], P('seq', 'tp'), may hold values from -0.09375 to 0.09375
- out_weight: bfloat16 [4096, 4096], P('seq', 'tp'), may hold values from -0.09375 to 0.09375
Outputs:
- mixed_out: bfloat16 [4096, 4096], P('seq', 'tp')
The draws below stay inside these ranges and needn't reach their ends.
Inputs may be any that keep to these rules, and one draw needn't show every extreme that they name: `decay_rate`: every entry is positive and below 0.034.
All inputs are finite; a program needn't handle non-finite values.
Results may differ from the reference program's by a relative error of at most 0.01.
Values may be sent and summed in bfloat16 or wider, within the bound.
A program may use at most 192 MiB of HBM per device.

```python
import jax
import jax.numpy as jnp
from jax import lax

D = 4096
H = 16
TOKENS = 4096


def draw_decay_rate(key, part):
    key_rate = jax.random.fold_in(key, 11)
    spread = jax.random.uniform(key_rate, (D, H), jnp.float32)
    lowest = jnp.log(0.5 / TOKENS)
    highest = jnp.log(1.0 / 30.0)
    rate_draw = jnp.exp(lowest + spread * (highest - lowest))
    return rate_draw


def level_of(stream_key, extent, split, least, top_value):
    level, own = 1.0, jax.random.fold_in(stream_key, 6)
    for position, shards_of in split:
        steps = jnp.exp(jax.random.uniform(jax.random.fold_in(own, position), (shards_of,), jnp.float32, least / len(split), top_value / len(split)))
        level = level * jnp.repeat(steps, extent[position] // shards_of).reshape([-1 if axis == position else 1 for axis in range(len(extent))])
    return level


def noise(own_key, dims, scale, bound, cuts=(), kind=jnp.bfloat16):
    loudness = level_of(own_key, dims, cuts, -0.22, 0.18) if cuts else 1.0
    drawn = jax.random.normal(own_key, dims, jnp.float32) * scale * loudness
    return jnp.minimum(jnp.maximum(drawn, -bound), bound).astype(kind)


def setup_inputs(seed: int = 0) -> dict:
    keys = jax.random.split(jax.random.key(seed), 9)
    return {
        "tokens": noise(keys[0], (TOKENS, D), 1.0, 6.0, ((0, 16), (1, 2))),
        "decay_rate": draw_decay_rate(jax.random.fold_in(keys[8], 71), 0),
        "angle": jnp.clip(jax.random.uniform(keys[2], (D, H), jnp.float32, -3.140625, 3.140625), -3.140625, 3.140625),
        "in_coef": noise(keys[3], (D, H), 1.0, 4.0, ((0, 2),), jnp.float32),
        "out_coef": noise(keys[4], (2, D, H), H ** -0.5, 1.5, ((1, 2),), jnp.float32),
        "skip_coef": jnp.clip(0.3 + 1.2 * jax.random.uniform(keys[5], (D,), jnp.float32) ** level_of(keys[5], (D,), ((0, 2),), -0.2, 0.2), 0.3, 1.5),
        "gate_weight": noise(keys[6], (D, D), D ** -0.5, 0.09375, ((0, 16), (1, 2))),
        "out_weight": noise(keys[7], (D, D), D ** -0.5, 0.09375, ((0, 16), (1, 2))),
    }


def kernel_block(rate, rotation_rate, in_part, out_real, out_imag, length):
    positions = jnp.arange(length).astype(jnp.float32)[:, None, None]
    magnitude = 1.0 - rate
    scaled = in_part * jnp.sqrt(1.0 - magnitude * magnitude)
    damping = jnp.exp(positions * jnp.log1p(-rate))
    rotation = positions * rotation_rate
    summands = scaled * damping * (out_real * jnp.cos(rotation) - out_imag * jnp.sin(rotation))
    return lax.optimization_barrier(jnp.sum(summands, axis=2))

def reference(tokens, decay_rate, angle, in_coef, out_coef, skip_coef, gate_weight, out_weight):
    length = tokens.shape[0]
    channels = tokens.shape[1]
    group_size = min(128, channels)
    group_count = channels // group_size
    values = tokens.astype(jnp.float32)

    def per_group(group_index):
        offset = group_index * group_size
        columns = lax.dynamic_slice_in_dim(values, offset, group_size, 1)

        def select(table):
            return lax.dynamic_slice_in_dim(table, offset, group_size, 0)
        kernel = kernel_block(select(decay_rate), select(angle), select(in_coef), select(out_coef[0]), select(out_coef[1]), length)
        spectrum = jnp.fft.rfft(columns, n=2 * length, axis=0) * jnp.fft.rfft(kernel, n=2 * length, axis=0)
        return jnp.fft.irfft(spectrum, n=2 * length, axis=0)[:length]
    blocks = lax.map(per_group, jnp.arange(group_count, dtype=jnp.int32))
    smoothed = jnp.transpose(blocks, (1, 0, 2)).reshape(length, channels) + skip_coef * values
    gate_pre = jnp.dot(tokens, gate_weight, preferred_element_type=jnp.float32)
    hidden = (jax.nn.silu(smoothed) * jax.nn.sigmoid(gate_pre)).astype(jnp.bfloat16)
    return jnp.dot(hidden, out_weight, preferred_element_type=jnp.float32).astype(jnp.bfloat16)
```

```python
import jax
import jax.numpy as jnp
from jax import lax
from jax.experimental import pallas as pl
from jax.experimental.pallas import tpu as pltpu
from jax.sharding import PartitionSpec as P

LANES = 128
UNROLL = 8
PIECE_BYTES = 512 * 1024


def small_gather(array, name, axis, split_axis):
    count = lax.axis_size(name)
    total = array.size * array.dtype.itemsize * count
    pieces = max(1, total // PIECE_BYTES)
    while array.shape[split_axis] % pieces:
        pieces -= 1
    parts = jnp.split(array, pieces, axis=split_axis)
    done = [lax.all_gather(part, name, axis=axis, tiled=True) for part in parts]
    return done[0] if pieces == 1 else jnp.concatenate(done, axis=split_axis)


def step_state(state, values, q_re, q_im):
    advanced = []
    for (re, im), a, b in zip(state, q_re, q_im):
        advanced.append((a * re - b * im + values, a * im + b * re))
    return advanced


def end_kernel(x_ref, q_re_ref, q_im_ref, end_re_ref, end_im_ref):
    dims = q_re_ref.shape[0]
    q_re = [q_re_ref[h] for h in range(dims)]
    q_im = [q_im_ref[h] for h in range(dims)]
    zero = jnp.zeros(q_re[0].shape, jnp.float32)

    def body(i, state):
        for u in range(UNROLL):
            state = step_state(state, x_ref[i * UNROLL + u], q_re, q_im)
        return state

    state = lax.fori_loop(0, x_ref.shape[0] // UNROLL, body, [(zero, zero)] * dims)
    for h in range(dims):
        end_re_ref[h] = state[h][0]
        end_im_ref[h] = state[h][1]


def smooth_kernel(
    position_ref, x_ref, q_re_ref, q_im_ref, c_re_ref, c_im_ref, span_re_ref, span_im_ref,
    ends_re_ref, ends_im_ref, skip_ref, y_ref,
):
    dims = q_re_ref.shape[0]
    zero = jnp.zeros(q_re_ref.shape[1:], jnp.float32)

    def horner(k, state):
        moved = []
        for h in range(dims):
            re, im = state[h]
            a, b = span_re_ref[h], span_im_ref[h]
            moved.append((
                a * re - b * im + ends_re_ref[k, h].astype(jnp.float32),
                a * im + b * re + ends_im_ref[k, h].astype(jnp.float32),
            ))
        return moved

    state = lax.fori_loop(0, position_ref[0], horner, [(zero, zero)] * dims)
    q_re = [q_re_ref[h] for h in range(dims)]
    q_im = [q_im_ref[h] for h in range(dims)]
    c_re = [c_re_ref[h] for h in range(dims)]
    c_im = [c_im_ref[h] for h in range(dims)]

    @pl.when(pl.program_id(1) == 0)
    def _():
        y_ref[...] = x_ref[...] * skip_ref[...][None]

    def body(i, state):
        for u in range(UNROLL):
            t = i * UNROLL + u
            state = step_state(state, x_ref[t], q_re, q_im)
            sums = [c_re[h] * state[h][0] - c_im[h] * state[h][1] for h in range(dims)]
            while len(sums) > 1:
                sums = [sum(sums[k:k + 2]) for k in range(0, len(sums), 2)]
            y_ref[t] += sums[0]
        return state

    lax.fori_loop(0, x_ref.shape[0] // UNROLL, body, state)


def per_device(tokens, decay_rate, angle, in_coef, out_coef, skip_coef, gate_weight, out_weight):
    rows, channels = tokens.shape
    dims = decay_rate.shape[1]
    tiles = channels // LANES
    sub = 8 if tiles % 8 == 0 else tiles
    half = dims // 2 if dims % 2 == 0 else dims
    grid = (tiles // sub, dims // half)

    gate_all = lax.all_gather(gate_weight, "seq", axis=0, tiled=True)
    out_all = lax.all_gather(out_weight, "seq", axis=0, tiled=True)

    def spread(table):
        return table.T.reshape(dims, tiles, LANES)

    rate = spread(decay_rate)
    theta = spread(angle)
    magnitude = 1.0 - rate
    scaled = spread(in_coef) * jnp.sqrt(1.0 - magnitude * magnitude)
    c_re = scaled * spread(out_coef[0])
    c_im = scaled * spread(out_coef[1])
    q_re = magnitude * jnp.cos(theta)
    q_im = magnitude * jnp.sin(theta)
    span_mag = jnp.exp(rows * jnp.log1p(-rate))
    span_re = span_mag * jnp.cos(rows * theta)
    span_im = span_mag * jnp.sin(rows * theta)
    values = tokens.astype(jnp.float32).reshape(rows, tiles, LANES)

    x_spec = pl.BlockSpec((rows, sub, LANES), lambda g, h: (0, g, 0))
    table_spec = pl.BlockSpec((half, sub, LANES), lambda g, h: (h, g, 0))
    table_shape = jax.ShapeDtypeStruct((dims, tiles, LANES), jnp.float32)
    end_re, end_im = pl.pallas_call(
        end_kernel,
        grid=grid,
        in_specs=[x_spec, table_spec, table_spec],
        out_specs=[table_spec, table_spec],
        out_shape=[table_shape, table_shape],
        name="end_state",
    )(values, q_re, q_im)

    columns = small_gather(tokens, "tp", 1, 0)
    ends_re = small_gather(end_re.astype(jnp.bfloat16)[None], "seq", 0, 1)
    ends_im = small_gather(end_im.astype(jnp.bfloat16)[None], "seq", 0, 1)
    devices = ends_re.shape[0]
    ends_spec = pl.BlockSpec((devices, half, sub, LANES), lambda g, h: (0, h, g, 0))
    position = lax.axis_index("seq").astype(jnp.int32).reshape(1)
    smoothed = pl.pallas_call(
        smooth_kernel,
        grid=grid,
        in_specs=[pl.BlockSpec(memory_space=pltpu.SMEM), x_spec]
        + [table_spec] * 6
        + [ends_spec, ends_spec, pl.BlockSpec((sub, LANES), lambda g, h: (g, 0))],
        out_specs=x_spec,
        out_shape=jax.ShapeDtypeStruct((rows, tiles, LANES), jnp.float32),
        name="smooth",
    )(
        position, values, q_re, q_im, c_re, c_im, span_re, span_im, ends_re, ends_im,
        skip_coef.reshape(tiles, LANES),
    ).reshape(rows, channels)
    activated = jax.nn.silu(smoothed)
    gate_pre = jnp.dot(columns, gate_all, preferred_element_type=jnp.float32)
    hidden = (activated * jax.nn.sigmoid(gate_pre)).astype(jnp.bfloat16)
    hidden_all = small_gather(hidden, "tp", 1, 0)
    mixed_out = jnp.dot(hidden_all, out_all, preferred_element_type=jnp.float32)
    return mixed_out.astype(jnp.bfloat16)


def solution(mesh):
    in_specs = (
        P("seq", "tp"),
        P("tp", None),
        P("tp", None),
        P("tp", None),
        P(None, "tp", None),
        P("tp"),
        P("seq", "tp"),
        P("seq", "tp"),
    )
    return jax.shard_map(
        per_device, mesh=mesh, in_specs=in_specs, out_specs=P("seq", "tp"), check_vma=False
    )
```
